32 devices in a mesh: grp: 2 (over y), seq: 16 (over z, x, core).
Axes of the slice: x: 2, y: 2, z: 4, core: 2. Of those that a mesh axis runs over, the one named last changes fastest.
Arguments:
- history: bfloat16 [8192, 1024], P(('grp', 'seq')), parts along dimension 0, may hold values from -6 to 6
- candidates: bfloat16 [512, 1024], P(('grp', 'seq')), parts along dimension 0, may hold values from -6 to 6
- lengths: int32 [8], P('grp'), parts along dimension 0, may hold values from 1 to 2048, 4096 in all
- cand_user: int32 [512], P(('grp', 'seq')), parts along dimension 0, may hold values from 0 to 3
- w_in: bfloat16 [1, 1024, 4096], replicated, may hold values from -0.125 to 0.125
- w_out: bfloat16 [1, 1024, 1024], replicated, may hold values from -0.1875 to 0.1875
Outputs:
- history_out: bfloat16 [8192, 1024], P(('grp', 'seq')), parts along dimension 0
- cand_out: bfloat16 [512, 1024], P(('grp', 'seq')), parts along dimension 0
The draws below stay inside these ranges and needn't reach their ends.
There are 2 independent parts, one for each index of `grp`. The reference program is written for one: setup_inputs(seed, part) draws one part's arguments, and reference() takes and returns one part's arrays. A program takes and returns all parts, laid end to end along the dimension named above; an argument that names none is the same for every part. Nothing has to cross between parts.
Inputs may be any that keep to these rules, and one draw needn't show every extreme that they name: Each user's history length is at least 1; the lengths sum to 4096, and one of them is exactly 2048.
All inputs are finite; a program needn't handle non-finite values.
Results may differ from the reference program's by a relative error of at most 0.0075.
Values may be sent and summed in bfloat16 or wider, within the bound.
A program may use at most 128 MiB of HBM per device.

```python
import math
import jax
import jax.numpy as jnp
import numpy as np
from jax import lax

D = 1024
HEADS = 8
HEAD_DIM = 128
LAYERS = 1
TOK_DEV = 256
HIST = 4096
WIN = 8
SPAN = 1792
USERS = 4
MOSTLEN = 2048
CANDS = 256
N_SEQ = 16


def draw_w_in(key, part):
    noise_key = jax.random.fold_in(key, 11)
    head_key = jax.random.fold_in(key, 23)
    independent = jax.random.normal(noise_key, (LAYERS, D, 4 * D), jnp.float32)
    weight_share = 0.7
    common = jax.random.normal(head_key, (LAYERS, D, 2, HEADS, 1), jnp.float32)
    common = jnp.broadcast_to(common, (LAYERS, D, 2, HEADS, D // HEADS)).reshape(LAYERS, D, 2 * D)
    query_key = weight_share * common + (1.0 - weight_share * weight_share) ** 0.5 * independent[:, :, 2 * D:]
    complete = jnp.concatenate([independent[:, :, 0:2 * D], query_key], axis=2)
    return (jnp.clip(complete, -4.0, 4.0) * D ** (-0.5)).astype(jnp.bfloat16)


def with_ends(drawn, key, low, high):
    dims = drawn.shape
    spot = [jax.random.randint(jax.random.fold_in(key, axis), (), 0, dims[axis]) for axis in range(len(dims))]
    drawn = drawn.at[tuple(spot)].set(low)
    longest = dims.index(max(dims))
    spot[longest] = (spot[longest] + 1) % dims[longest]
    return drawn.at[tuple(spot)].set(high)


def block_levels(rng, extent, cuts, low, high):
    def one(axis_at, parts):
        steps = jax.random.uniform(jax.random.fold_in(jax.random.fold_in(rng, 6), axis_at), (parts,), jnp.float32, low / len(cuts), high / len(cuts))
        return jnp.repeat(jnp.exp(steps), extent[axis_at] // parts).reshape((-1,) + (1,) * (len(extent) - axis_at - 1))

    level = one(*cuts[0])
    for cut in cuts[1:]:
        level = level * one(*cut)
    return level


def profile(number_of, total, reach, skew):
    portions = [(1 << 20) // math.isqrt(standing ** skew) + 1 for standing in range(2, number_of + 1)]
    surplus, counts = total - reach - (number_of - 1), [1] * (number_of - 1)
    while surplus > 0:
        free = [i for i in range(number_of - 1) if counts[i] < reach]
        pool, left = sum([portions[i] for i in free]), surplus
        for i in free:
            addition = min(reach - counts[i], max(1, left * portions[i] // pool), surplus)
            counts[i] = counts[i] + addition
            surplus = surplus - addition
    return np.array([reach] + counts)


def ragged(rng, amount, total, most, lean):
    if amount == 2:
        one = jax.random.randint(rng, (), max(1, total - most), min(most, total - 1) + 1)
        return jnp.stack([one, total - one])
    sizes = jnp.asarray(profile(amount, total, most, lean), jnp.int32)
    couples = (amount - 1) // 2
    donor, receiver = sizes[1:1 + 2 * couples:2], sizes[2:2 + 2 * couples:2]
    slack = jnp.minimum(donor - 1, most - receiver)
    passed = jax.random.randint(jax.random.fold_in(rng, 1), (couples,), 0, 1 << 20) % (slack + 1)
    sizes = sizes.at[1:1 + 2 * couples:2].set(donor - passed).at[2:2 + 2 * couples:2].set(receiver + passed)
    return sizes[jax.random.permutation(jax.random.fold_in(rng, 2), amount)]


def noise(stream_key, dims, deviation, reach, split=(), kind=jnp.bfloat16):
    loudness = block_levels(stream_key, dims, split, -0.22, 0.18) if split else 1.0
    array = jax.random.normal(stream_key, dims, jnp.float32) * deviation * loudness
    return jnp.minimum(jnp.maximum(array, -reach), reach).astype(kind)


def setup_inputs(seed: int = 0, part: int = 0) -> dict:
    key_list = jax.random.split(jax.random.key(seed), 7)
    own_keys = jax.random.split(jax.random.fold_in(key_list[6], part), 7)
    history = noise(own_keys[0], (HIST, D), 1.0, 6.0, ((0, 16),))
    candidates = noise(own_keys[1], (CANDS, D), 1.0, 6.0, ((0, 16),))
    lengths = ragged(own_keys[2], USERS, HIST, MOSTLEN, 2).astype(jnp.int32)
    cand_user = with_ends(jax.random.randint(own_keys[3], (CANDS,), 0, USERS), jax.random.fold_in(own_keys[3], 1), 0, USERS - 1).astype(jnp.int32)
    w_in = draw_w_in(jax.random.fold_in(key_list[6], 71), part)
    w_out = noise(key_list[5], (LAYERS, D, D), D ** -0.5, 0.1875)
    return {"history": history, "candidates": candidates, "lengths": lengths, "cand_user": cand_user, "w_in": w_in, "w_out": w_out}


eps = 1e-06

def layer_norm(rows):
    centred = rows - lax.optimization_barrier(jnp.mean(rows, axis=-1, keepdims=True))
    return centred * lax.rsqrt(lax.optimization_barrier(jnp.mean(centred * centred, axis=-1, keepdims=True)) + eps)

def segment_of(positions, ends):
    return lax.optimization_barrier(jnp.sum((positions[:, None] >= ends[None, :]).astype(jnp.int32), axis=1)).astype(jnp.int32)

def reference(history, candidates, lengths, cand_user, w_in, w_out):
    ends = jnp.cumsum(lengths).astype(jnp.int32)
    scale = HEAD_DIM ** (-0.5)
    width = WIN * TOK_DEV
    x_rows = history
    c_rows = candidates
    all_seg = segment_of(jnp.arange(HIST, dtype=jnp.int32), ends)
    for layer in range(LAYERS):
        normed = layer_norm(x_rows.astype(jnp.float32)).astype(jnp.bfloat16)
        proj = jax.nn.silu(jnp.dot(normed, w_in[layer], preferred_element_type=jnp.float32)).astype(jnp.bfloat16)
        u_all = proj[:, 0:D]
        v_all = proj[:, D:2 * D]
        q_all = proj[:, 2 * D:3 * D]
        k_all = proj[:, 3 * D:4 * D]
        front = jnp.zeros(((WIN - 1) * TOK_DEV, D), jnp.bfloat16)
        k_pad = jnp.concatenate([front, k_all], axis=0)
        v_pad = jnp.concatenate([front, v_all], axis=0)

        def hist_block(block):
            first = (block * TOK_DEV).astype(jnp.int32)
            q_blk = lax.dynamic_slice_in_dim(q_all, first, TOK_DEV, 0).astype(jnp.float32).reshape(TOK_DEV, HEADS, HEAD_DIM)
            k_blk = lax.dynamic_slice_in_dim(k_pad, first, width, 0).astype(jnp.float32).reshape(width, HEADS, HEAD_DIM)
            v_blk = lax.dynamic_slice_in_dim(v_pad, first, width, 0).astype(jnp.float32).reshape(width, HEADS, HEAD_DIM)
            q_pos = first + jnp.arange(TOK_DEV, dtype=jnp.int32)
            k_pos = first - (WIN - 1) * TOK_DEV + jnp.arange(width, dtype=jnp.int32)
            allowed = (k_pos[None, :] >= 0) & (k_pos[None, :] <= q_pos[:, None])
            allowed = allowed & (q_pos[:, None] - k_pos[None, :] < SPAN)
            allowed = allowed & (segment_of(k_pos, ends)[None, :] == segment_of(q_pos, ends)[:, None])
            scores = jnp.einsum('qhd,khd->hqk', q_blk, k_blk) * scale
            weight = jnp.where(allowed[None], jax.nn.silu(scores), 0.0).astype(jnp.bfloat16)
            return jnp.einsum('hqk,khd->qhd', weight.astype(jnp.float32), v_blk).reshape(TOK_DEV, D)
        attn = lax.map(hist_block, jnp.arange(N_SEQ, dtype=jnp.int32)).reshape(HIST, D)
        y_rows = (layer_norm(attn) * u_all.astype(jnp.float32)).astype(jnp.bfloat16)
        x_rows = (x_rows.astype(jnp.float32) + jnp.dot(y_rows, w_out[layer], preferred_element_type=jnp.float32)).astype(jnp.bfloat16)
        cnormed = layer_norm(c_rows.astype(jnp.float32)).astype(jnp.bfloat16)
        u_c = jax.nn.silu(jnp.dot(cnormed, w_in[layer][:, 0:D], preferred_element_type=jnp.float32)).astype(jnp.bfloat16)
        q_c = jax.nn.silu(jnp.dot(cnormed, w_in[layer][:, 2 * D:3 * D], preferred_element_type=jnp.float32)).astype(jnp.bfloat16)
        cq_heads = q_c.astype(jnp.float32).reshape(CANDS, HEADS, HEAD_DIM)

        def cand_shard(block, total):
            first = (block * TOK_DEV).astype(jnp.int32)
            k_blk = lax.dynamic_slice_in_dim(k_all, first, TOK_DEV, 0).astype(jnp.float32).reshape(TOK_DEV, HEADS, HEAD_DIM)
            v_blk = lax.dynamic_slice_in_dim(v_all, first, TOK_DEV, 0).astype(jnp.float32).reshape(TOK_DEV, HEADS, HEAD_DIM)
            k_seg = lax.dynamic_slice_in_dim(all_seg, first, TOK_DEV, 0)
            owned = cand_user[:, None] == k_seg[None, :]
            scores = jnp.einsum('chd,khd->hck', cq_heads, k_blk) * scale
            weight = jnp.where(owned[None], jax.nn.silu(scores), 0.0).astype(jnp.bfloat16)
            return total + jnp.einsum('hck,khd->chd', weight.astype(jnp.float32), v_blk).reshape(CANDS, D)
        cattn = lax.fori_loop(0, N_SEQ, cand_shard, jnp.zeros((CANDS, D), jnp.float32))
        y_c = (layer_norm(cattn) * u_c.astype(jnp.float32)).astype(jnp.bfloat16)
        c_rows = (c_rows.astype(jnp.float32) + jnp.dot(y_c, w_out[layer], preferred_element_type=jnp.float32)).astype(jnp.bfloat16)
    return (x_rows, c_rows)
```

```python
import functools

import jax
import jax.numpy as jnp
from jax import lax
from jax.experimental import pallas as pl
from jax.experimental.pallas import tpu as pltpu
from jax.sharding import PartitionSpec as P

HEADS = 8
WIN = 8
CHUNKS = 2
ROW = 4

eps = 1e-06
bf16 = jnp.bfloat16
f32 = jnp.float32


def layer_norm(rows):
    centred = rows - jnp.mean(rows, axis=-1, keepdims=True)
    return centred * lax.rsqrt(jnp.mean(centred * centred, axis=-1, keepdims=True) + eps)


def silu_of_twice(half):
    return half + half * jnp.tanh(half)


def dot(a, b):
    return jnp.dot(a, b, preferred_element_type=f32)


def dot_t(a, b):
    return lax.dot_general(a, b, (((1,), (1,)), ((), ())), preferred_element_type=f32)


def kernel(
    n,
    lengths,
    hist,
    cand,
    users,
    w_in_hbm,
    w_out_hbm,
    out_ref,
    cout_ref,
    w_in,
    w_out,
    wnd,
    q_s,
    u_s,
    kv_s,
    own_kv,
    acc,
    cbuf,
    ubuf,
    qc_s,
    part,
    buf1,
    buf2,
    buf3,
    w_sem,
    x_send,
    x_recv,
    cz_send,
    cz_recv,
    uz_send,
    uz_recv,
    cx_send,
    cx_recv,
    rz_send,
    rz_recv,
):
    rows, width = hist.shape
    cr = cand.shape[0]
    head_dim = width // HEADS
    half_scale = 0.5 * head_dim ** (-0.5)
    depth = n // ROW
    s = lax.axis_index("seq")
    z = s // ROW
    r = s % ROW
    p = r // 2
    k = r % 2
    piece = rows // CHUNKS
    sibling = s + 1 - 2 * k
    partner = s + 2 - 4 * p

    w_copies = [
        pltpu.make_async_copy(
            w_in_hbm.at[0, :, pl.ds(c * width, width)], w_in.at[c], w_sem.at[c]
        )
        for c in range(4)
    ]
    w_copies.append(pltpu.make_async_copy(w_out_hbm.at[0], w_out, w_sem.at[4]))
    for c in (2, 3, 1, 0, 4):
        w_copies[c].start()

    barrier = pltpu.get_barrier_semaphore()
    pl.semaphore_signal(barrier, inc=1, device_id={"seq": sibling}, device_id_type=pl.DeviceIdType.MESH)
    pl.semaphore_signal(barrier, inc=1, device_id={"seq": partner}, device_id_type=pl.DeviceIdType.MESH)

    def greet(d, carry):
        pl.semaphore_signal(
            barrier,
            inc=1,
            device_id={"seq": (s + ROW * d) % n},
            device_id_type=pl.DeviceIdType.MESH,
        )
        return carry

    lax.fori_loop(1, depth, greet, 0)
    pl.semaphore_wait(barrier, depth + 1)

    def remote(src, dst, send, recv, to):
        return pltpu.make_async_remote_copy(
            src_ref=src,
            dst_ref=dst,
            send_sem=send,
            recv_sem=recv,
            device_id={"seq": to},
            device_id_type=pl.DeviceIdType.MESH,
        )

    def x_copy(src_slot, dst_slot, h, kind, to):
        part_rows = pl.ds(h * piece, piece)
        src = hist.at[part_rows] if src_slot is None else wnd.at[src_slot, part_rows]
        return remote(src, wnd.at[dst_slot, part_rows], x_send.at[kind, h], x_recv.at[dst_slot, h], to)

    own_slot = 2 * ROW + r
    up = (s + ROW) % n

    me_block = k * 2 + p

    def cz_copy(d, which):
        to = (s + ROW * d) % n
        at = pl.ds(pl.multiple_of(z * cr, cr), cr)
        if which == 0:
            return remote(cand, cbuf.at[me_block, at], cz_send.at[d], cz_recv.at[d], to)
        return remote(users, ubuf.at[me_block, at], uz_send.at[d], uz_recv.at[d], to)

    def cz_start(d, carry):
        cz_copy(d, 0).start()
        cz_copy(d, 1).start()
        return carry

    lax.fori_loop(1, depth, cz_start, 0)

    for h in range(CHUNKS):

        @pl.when(z + 1 < depth)
        def _():
            x_copy(None, ROW + r, h, 0, up).start()

        @pl.when(p == 0)
        def _():
            x_copy(None, own_slot, h, 1, partner).start()

        @pl.when(k == 0)
        def _():
            x_copy(None, own_slot, h, 2, sibling).start()

    ends = []
    total = jnp.int32(0)
    for j in range(lengths.shape[0]):
        total = total + lengths[j]
        ends.append(total)

    def seg(pos):
        out = jnp.zeros(pos.shape, jnp.int32)
        for e in ends:
            out = out + (pos >= e).astype(jnp.int32)
        return out

    q_pos = s * rows + lax.broadcasted_iota(jnp.int32, (rows, 1), 0)
    q_seg = seg(q_pos)

    def project(normed, block):
        return silu_of_twice(dot(normed, w_in[block]) * 0.5).astype(bf16)

    def attend(kv, shard):
        k_pos = shard * rows + lax.broadcasted_iota(jnp.int32, (1, rows), 1)
        ok = (k_pos <= q_pos) & (q_pos - k_pos < (WIN - 1) * rows) & (seg(k_pos) == q_seg)
        for h in range(HEADS):
            cols = slice(h * head_dim, (h + 1) * head_dim)
            half = dot_t(q_s[:, cols], kv[0, :, cols]) * half_scale
            weight = jnp.where(ok, silu_of_twice(half), 0.0).astype(bf16)
            acc[:, cols] += dot(weight, kv[1, :, cols])

    acc[...] = jnp.zeros_like(acc)
    normed = layer_norm(hist[...].astype(f32)).astype(bf16)
    w_copies[2].wait()
    q_s[...] = project(normed, 2)
    w_copies[3].wait()
    own_kv[0] = project(normed, 3)

    mine_at = pl.ds(pl.multiple_of(z * cr, cr), cr)
    cbuf[me_block, mine_at] = cand[...]
    ubuf[me_block, mine_at] = users[...]

    def cz_wait(d, carry):
        cz_copy(d, 0).wait_recv()
        cz_copy(d, 1).wait_recv()
        return carry

    lax.fori_loop(1, depth, cz_wait, 0)
    to_partner = [
        remote(cbuf.at[me_block], cbuf.at[me_block], cx_send.at[0], cx_recv.at[0], partner),
        remote(ubuf.at[me_block], ubuf.at[me_block], cx_send.at[1], cx_recv.at[1], partner),
    ]
    for c in to_partner:
        c.start()
    w_copies[1].wait()
    own_kv[1] = project(normed, 1)
    for c in to_partner:
        c.wait_recv()
    to_sibling = [
        remote(cbuf.at[pl.ds(2 * k, 2)], cbuf.at[pl.ds(2 * k, 2)], cx_send.at[2], cx_recv.at[2], sibling),
        remote(ubuf.at[pl.ds(2 * k, 2)], ubuf.at[pl.ds(2 * k, 2)], cx_send.at[3], cx_recv.at[3], sibling),
    ]
    for c in to_sibling:
        c.start()
    w_copies[0].wait()
    u_s[...] = project(normed, 0)
    attend(own_kv, s)
    for c in to_sibling:
        c.wait_recv()

    def red1():
        return remote(part.at[pl.ds(2 - 2 * k, 2)], buf1, cx_send.at[4], cx_recv.at[4], sibling)

    def red2():
        return remote(part.at[k * 2 + 1 - p], buf2, cx_send.at[5], cx_recv.at[5], partner)

    def red3(d):
        to_row = (z + d) % depth
        src = part.at[me_block, pl.ds(pl.multiple_of(to_row * cr, cr), cr)]
        return remote(src, buf3.at[d], rz_send.at[d], rz_recv.at[d], (s + ROW * d) % n)

    block_rows = depth * cr
    k_row = s * rows + lax.broadcasted_iota(jnp.int32, (1, rows), 1)
    k_seg = seg(k_row)

    def cand_scores(first, count):
        size = count * block_rows
        c_norm = layer_norm(cbuf[pl.ds(first, count)].reshape(size, width).astype(f32)).astype(bf16)
        qc_s[...] = project(c_norm, 2)
        owner = ubuf[pl.ds(first, count)].reshape(size, ubuf.shape[-1])[:, :1]
        ok = owner == k_seg
        for h in range(HEADS):
            cols = slice(h * head_dim, (h + 1) * head_dim)
            half = dot_t(qc_s[:, cols], own_kv[0, :, cols]) * half_scale
            weight = jnp.where(ok, silu_of_twice(half), 0.0).astype(bf16)
            part[pl.ds(first, count), :, cols] = dot(weight, own_kv[1, :, cols]).reshape(
                count, block_rows, head_dim
            )

    count = qc_s.shape[0] // block_rows
    if count == ROW:
        cand_scores(0, ROW)
    else:

        def cand_block(b, carry):
            cand_scores(b * count, count)
            return carry

        lax.fori_loop(0, ROW // count, cand_block, 0)
    red1().start()

    def needed(slot, of):
        return (slot > of) & (slot < 2 * ROW + of) & (z - 2 + slot // ROW >= 0)

    def pair(j, carry):
        base = 2 * ROW - ROW * (j // 2)
        swap = jnp.minimum(j // 2, 1) * p
        first = base + 2 * ((j + swap) % 2)
        mine = first + k

        def hop(h, go_up, go_across):
            pieces = pl.ds(h * piece, piece)
            pltpu.make_async_copy(hist.at[pieces], wnd.at[mine, pieces], x_recv.at[mine, h]).wait()
            if go_up:

                @pl.when((z + 1 < depth) & (r >= 1))
                def _():
                    x_copy(mine, mine - ROW, h, 3, up).start()

            if go_across == 1:
                x_copy(mine, mine, h, 4, partner).start()
            if go_across == 2:

                @pl.when(p == 1)
                def _():
                    x_copy(mine, mine, h, 5, partner).start()

            @pl.when(needed(mine, r + 1 - 2 * k))
            def _():
                x_copy(mine, mine, h, 6 + j, sibling).start()

        @pl.when((j == 0) & (p == 1))
        def _():
            for h in range(CHUNKS):
                hop(h, False, 0)

        @pl.when((j == 2) & (z >= 1))
        def _():
            for h in range(CHUNKS):
                hop(h, True, 1)

        @pl.when((j == 3) & (z >= 1))
        def _():
            for h in range(CHUNKS):
                hop(h, False, 0)

        @pl.when((j == 4) & (z >= 2) & (r >= 1))
        def _():
            for h in range(CHUNKS):
                hop(h, False, 2)

        @pl.when((j == 5) & (z >= 2) & (p == 0))
        def _():
            for h in range(CHUNKS):
                hop(h, False, 0)

        @pl.when(j == 2)
        def _():
            red1().wait_recv()
            part[pl.ds(2 * k, 2)] += buf1[...]
            red2().start()

        @pl.when(j == 3)
        def _():
            red2().wait_recv()
            part[me_block] += buf2[...]

            def send(d, c):
                red3(d).start()
                return c

            lax.fori_loop(1, depth, send, 0)

        def one(m, c):
            slot = first + (k + m) % 2

            @pl.when(needed(slot, r))
            def _():
                @pl.when(m == 1)
                def _():
                    for h in range(CHUNKS):
                        pieces = pl.ds(h * piece, piece)
                        pltpu.make_async_copy(
                            hist.at[pieces], wnd.at[slot, pieces], x_recv.at[slot, h]
                        ).wait()

                norm = layer_norm(wnd[slot].astype(f32)).astype(bf16)
                kv_s[0] = project(norm, 3)
                kv_s[1] = project(norm, 1)
                attend(kv_s, (z - 2) * ROW + slot)

            return c

        return lax.fori_loop(0, 2, one, carry)

    lax.fori_loop(0, 6, pair, 0)

    w_copies[4].wait()
    y = (layer_norm(acc[...]) * u_s[...].astype(f32)).astype(bf16)
    out_ref[...] = (hist[...].astype(f32) + dot(y, w_out[...])).astype(bf16)

    u_c = project(layer_norm(cand[...].astype(f32)).astype(bf16), 0)

    def take(d, c):
        red3(d).wait_recv()
        return c + buf3[d]

    mine_sum = part[me_block, mine_at]
    cattn = lax.fori_loop(1, depth, take, mine_sum)
    y_c = (layer_norm(cattn) * u_c.astype(f32)).astype(bf16)
    cout_ref[...] = (cand[...].astype(f32) + dot(y_c, w_out[...])).astype(bf16)

    for c in to_partner + to_sibling + [red1(), red2()]:
        c.wait_send()

    def left(d, c):
        cz_copy(d, 0).wait_send()
        cz_copy(d, 1).wait_send()
        red3(d).wait_send()
        return c

    lax.fori_loop(1, depth, left, 0)
    for h in range(CHUNKS):

        @pl.when(z + 1 < depth)
        def _():
            x_copy(None, ROW + r, h, 0, up).wait_send()

        @pl.when(p == 0)
        def _():
            x_copy(None, own_slot, h, 1, partner).wait_send()

        @pl.when(k == 0)
        def _():
            x_copy(None, own_slot, h, 2, sibling).wait_send()

        @pl.when((z >= 1) & (z + 1 < depth) & (r >= 1))
        def _():
            x_copy(ROW + r, r, h, 3, up).wait_send()

        @pl.when(z >= 1)
        def _():
            x_copy(ROW + r, ROW + r, h, 4, partner).wait_send()

        @pl.when((z >= 2) & (p == 1))
        def _():
            x_copy(r, r, h, 5, partner).wait_send()

        other = r + 1 - 2 * k
        across = 2 * (1 - p) + k

        @pl.when((p == 1) & needed(2 * ROW + k, other))
        def _():
            x_copy(2 * ROW + k, 2 * ROW + k, h, 6, sibling).wait_send()

        @pl.when((z >= 1) & needed(ROW + r, other))
        def _():
            x_copy(ROW + r, ROW + r, h, 8, sibling).wait_send()

        @pl.when((z >= 1) & needed(ROW + across, other))
        def _():
            x_copy(ROW + across, ROW + across, h, 9, sibling).wait_send()

        @pl.when((z >= 2) & (r >= 1) & needed(r, other))
        def _():
            x_copy(r, r, h, 10, sibling).wait_send()

        @pl.when((z >= 2) & (p == 0) & needed(across, other))
        def _():
            x_copy(across, across, h, 11, sibling).wait_send()


def per_device(n, history, candidates, lengths, cand_user, w_in, w_out):
    rows, width = history.shape
    cr = candidates.shape[0]
    depth = n // ROW
    users = jnp.broadcast_to(cand_user[:, None], (cr, 128))
    vmem = pl.BlockSpec(memory_space=pltpu.VMEM)
    dma = pltpu.SemaphoreType.DMA
    block = depth * cr
    many = ROW * block if ROW * block <= 512 else block
    return pl.pallas_call(
        functools.partial(kernel, n),
        out_shape=(
            jax.ShapeDtypeStruct((rows, width), bf16),
            jax.ShapeDtypeStruct((cr, width), bf16),
        ),
        in_specs=[
            pl.BlockSpec(memory_space=pltpu.SMEM),
            vmem,
            vmem,
            vmem,
            pl.BlockSpec(memory_space=pl.ANY),
            pl.BlockSpec(memory_space=pl.ANY),
        ],
        out_specs=(vmem, vmem),
        scratch_shapes=[
            pltpu.VMEM((4, width, width), bf16),
            pltpu.VMEM((width, width), bf16),
            pltpu.VMEM((3 * ROW, rows, width), bf16),
            pltpu.VMEM((rows, width), bf16),
            pltpu.VMEM((rows, width), bf16),
            pltpu.VMEM((2, rows, width), bf16),
            pltpu.VMEM((2, rows, width), bf16),
            pltpu.VMEM((rows, width), f32),
            pltpu.VMEM((ROW, block, width), bf16),
            pltpu.VMEM((ROW, block, 128), jnp.int32),
            pltpu.VMEM((many, width), bf16),
            pltpu.VMEM((ROW, block, width), f32),
            pltpu.VMEM((2, block, width), f32),
            pltpu.VMEM((block, width), f32),
            pltpu.VMEM((depth, cr, width), f32),
            dma((5,)),
            dma((12, CHUNKS)),
            dma((3 * ROW, CHUNKS)),
            dma((depth,)),
            dma((depth,)),
            dma((depth,)),
            dma((depth,)),
            dma((6,)),
            dma((6,)),
            dma((depth,)),
            dma((depth,)),
        ],
        compiler_params=pltpu.CompilerParams(
            collective_id=0, has_side_effects=True, vmem_limit_bytes=60 * 1024 * 1024
        ),
    )(lengths, history, candidates, users, w_in, w_out)


def solution(mesh):
    n = mesh.shape["seq"]
    placed = (
        P(("grp", "seq"), None),
        P(("grp", "seq"), None),
        P("grp"),
        P(("grp", "seq")),
        P(),
        P(),
    )
    return jax.shard_map(
        functools.partial(per_device, n),
        mesh=mesh,
        in_specs=placed,
        out_specs=(P(("grp", "seq"), None), P(("grp", "seq"), None)),
        check_vma=False,
    )
```

```python
import functools

import jax
import jax.numpy as jnp
from jax import lax
from jax.experimental import pallas as pl
from jax.experimental.pallas import tpu as pltpu
from jax.sharding import PartitionSpec as P

HEADS = 8
WIN = 8
CHUNKS = 2
ROW = 4

eps = 1e-06
bf16 = jnp.bfloat16
f32 = jnp.float32


def layer_norm(rows):
    centred = rows - jnp.mean(rows, axis=-1, keepdims=True)
    return centred * lax.rsqrt(jnp.mean(centred * centred, axis=-1, keepdims=True) + eps)


def silu_of_twice(half):
    return half + half * jnp.tanh(half)


def dot(a, b):
    return jnp.dot(a, b, preferred_element_type=f32)


def dot_t(a, b):
    return lax.dot_general(a, b, (((1,), (1,)), ((), ())), preferred_element_type=f32)


def kernel(
    n,
    lengths,
    hist,
    cand,
    users_row,
    w_in_hbm,
    w_out_hbm,
    out_ref,
    cout_ref,
    w_in,
    w_out,
    wnd,
    q_s,
    u_s,
    kv_s,
    own_kv,
    acc,
    cbuf,
    ubuf,
    qc_s,
    part,
    buf1,
    buf2,
    buf3,
    out2,
    out3,
    users,
    w_sem,
    x_send,
    x_recv,
    cz_send,
    cz_recv,
    uz_send,
    uz_recv,
    cx_send,
    cx_recv,
    rz_send,
    rz_recv,
):
    rows, width = hist.shape
    cr = cand.shape[0]
    head_dim = width // HEADS
    half_scale = 0.5 * head_dim ** (-0.5)
    depth = n // ROW
    s = lax.axis_index("seq")
    z = s // ROW
    r = s % ROW
    p = r // 2
    k = r % 2
    piece = rows // CHUNKS
    sibling = s + 1 - 2 * k
    partner = s + 2 - 4 * p

    w_copies = [
        pltpu.make_async_copy(
            w_in_hbm.at[0, :, pl.ds(c * width, width)], w_in.at[c], w_sem.at[c]
        )
        for c in range(4)
    ]
    w_copies.append(pltpu.make_async_copy(w_out_hbm.at[0], w_out, w_sem.at[4]))
    for c in (2, 3, 1, 0, 4):
        w_copies[c].start()

    eye = lax.broadcasted_iota(jnp.int32, (cr, cr), 0) == lax.broadcasted_iota(jnp.int32, (cr, cr), 1)
    column = jnp.sum(jnp.where(eye, users_row[...], 0), axis=1, keepdims=True)
    users[...] = jnp.broadcast_to(column, users.shape)

    barrier = pltpu.get_barrier_semaphore()
    pl.semaphore_signal(barrier, inc=1, device_id={"seq": sibling}, device_id_type=pl.DeviceIdType.MESH)
    pl.semaphore_signal(barrier, inc=1, device_id={"seq": partner}, device_id_type=pl.DeviceIdType.MESH)

    def greet(d, carry):
        pl.semaphore_signal(
            barrier,
            inc=1,
            device_id={"seq": (s + ROW * d) % n},
            device_id_type=pl.DeviceIdType.MESH,
        )
        return carry

    lax.fori_loop(1, depth, greet, 0)
    pl.semaphore_wait(barrier, depth + 1)

    def remote(src, dst, send, recv, to):
        return pltpu.make_async_remote_copy(
            src_ref=src,
            dst_ref=dst,
            send_sem=send,
            recv_sem=recv,
            device_id={"seq": to},
            device_id_type=pl.DeviceIdType.MESH,
        )

    def x_copy(src_slot, dst_slot, h, kind, to):
        part_rows = pl.ds(h * piece, piece)
        src = hist.at[part_rows] if src_slot is None else wnd.at[src_slot, part_rows]
        return remote(src, wnd.at[dst_slot, part_rows], x_send.at[kind, h], x_recv.at[dst_slot, h], to)

    own_slot = 2 * ROW + r
    up = (s + ROW) % n

    me_block = k * 2 + p

    def cz_copy(d, which):
        to = (s + ROW * d) % n
        at = pl.ds(pl.multiple_of(z * cr, cr), cr)
        if which == 0:
            return remote(cand, cbuf.at[me_block, at], cz_send.at[d], cz_recv.at[d], to)
        return remote(users, ubuf.at[me_block, at], uz_send.at[d], uz_recv.at[d], to)

    def cz_start(d, carry):
        cz_copy(d, 0).start()
        cz_copy(d, 1).start()
        return carry

    lax.fori_loop(1, depth, cz_start, 0)

    for h in range(CHUNKS):

        @pl.when(z + 1 < depth)
        def _():
            x_copy(None, ROW + r, h, 0, up).start()

        @pl.when(k == 0)
        def _():
            x_copy(None, own_slot, h, 2, sibling).start()

    @pl.when(p == 0)
    def _():
        x_copy(None, own_slot, 0, 1, partner).start()

    ends = []
    total = jnp.int32(0)
    for j in range(lengths.shape[0]):
        total = total + lengths[j]
        ends.append(total)

    def seg(pos):
        out = jnp.zeros(pos.shape, jnp.int32)
        for e in ends:
            out = out + (pos >= e).astype(jnp.int32)
        return out

    q_pos = s * rows + lax.broadcasted_iota(jnp.int32, (rows, 1), 0)
    q_seg = seg(q_pos)

    def project(normed, block):
        return silu_of_twice(dot(normed, w_in[block]) * 0.5).astype(bf16)

    def attend(kv, shard):
        k_pos = shard * rows + lax.broadcasted_iota(jnp.int32, (1, rows), 1)
        ok = (k_pos <= q_pos) & (q_pos - k_pos < (WIN - 1) * rows) & (seg(k_pos) == q_seg)
        for h in range(HEADS):
            cols = slice(h * head_dim, (h + 1) * head_dim)
            half = dot_t(q_s[:, cols], kv[0, :, cols]) * half_scale
            weight = jnp.where(ok, silu_of_twice(half), 0.0).astype(bf16)
            acc[:, cols] += dot(weight, kv[1, :, cols])

    acc[...] = jnp.zeros_like(acc)
    normed = layer_norm(hist[...].astype(f32)).astype(bf16)
    w_copies[2].wait()
    q_s[...] = project(normed, 2)
    w_copies[3].wait()
    own_kv[0] = project(normed, 3)

    mine_at = pl.ds(pl.multiple_of(z * cr, cr), cr)
    cbuf[me_block, mine_at] = cand[...]
    ubuf[me_block, mine_at] = users[...]

    def cz_wait(d, carry):
        cz_copy(d, 0).wait_recv()
        cz_copy(d, 1).wait_recv()
        return carry

    lax.fori_loop(1, depth, cz_wait, 0)
    to_partner = [
        remote(cbuf.at[me_block], cbuf.at[me_block], cx_send.at[0], cx_recv.at[0], partner),
        remote(ubuf.at[me_block], ubuf.at[me_block], cx_send.at[1], cx_recv.at[1], partner),
    ]
    for c in to_partner:
        c.start()
    for h in range(1, CHUNKS):

        @pl.when(p == 0)
        def _():
            x_copy(None, own_slot, h, 1, partner).start()

    w_copies[1].wait()
    own_kv[1] = project(normed, 1)
    for c in to_partner:
        c.wait_recv()
    to_sibling = [
        remote(cbuf.at[pl.ds(2 * k, 2)], cbuf.at[pl.ds(2 * k, 2)], cx_send.at[2], cx_recv.at[2], sibling),
        remote(ubuf.at[pl.ds(2 * k, 2)], ubuf.at[pl.ds(2 * k, 2)], cx_send.at[3], cx_recv.at[3], sibling),
    ]
    for c in to_sibling:
        c.start()
    w_copies[0].wait()
    u_s[...] = project(normed, 0)
    attend(own_kv, s)
    for c in to_sibling:
        c.wait_recv()

    def red1():
        return remote(part.at[pl.ds(2 - 2 * k, 2)], buf1, cx_send.at[4], cx_recv.at[4], sibling)

    def red2():
        return remote(out2, buf2, cx_send.at[5], cx_recv.at[5], partner)

    def red3(d):
        to_row = (z + d) % depth
        src = out3.at[pl.ds(pl.multiple_of(to_row * cr, cr), cr)]
        return remote(src, buf3.at[d], rz_send.at[d], rz_recv.at[d], (s + ROW * d) % n)

    block_rows = depth * cr
    k_row = s * rows + lax.broadcasted_iota(jnp.int32, (1, rows), 1)
    k_seg = seg(k_row)

    def cand_scores(first, count):
        size = count * block_rows
        c_norm = layer_norm(cbuf[pl.ds(first, count)].reshape(size, width).astype(f32)).astype(bf16)
        qc_s[...] = project(c_norm, 2)
        owner = ubuf[pl.ds(first, count)].reshape(size, ubuf.shape[-1])[:, :1]
        ok = owner == k_seg
        for h in range(HEADS):
            cols = slice(h * head_dim, (h + 1) * head_dim)
            half = dot_t(qc_s[:, cols], own_kv[0, :, cols]) * half_scale
            weight = jnp.where(ok, silu_of_twice(half), 0.0).astype(bf16)
            part[pl.ds(first, count), :, cols] = dot(weight, own_kv[1, :, cols]).reshape(
                count, block_rows, head_dim
            )

    count = qc_s.shape[0] // block_rows
    if count == ROW:
        cand_scores(0, ROW)
    else:

        def cand_block(b, carry):
            cand_scores(b * count, count)
            return carry

        lax.fori_loop(0, ROW // count, cand_block, 0)
    red1().start()

    def needed(slot, of):
        return (slot > of) & (slot < 2 * ROW + of) & (z - 2 + slot // ROW >= 0)

    def pair_of(j):
        base = 2 * ROW - ROW * (j // 2)
        swap = min(j // 2, 1) * p if isinstance(j, int) else jnp.minimum(j // 2, 1) * p
        return base + 2 * ((j + swap) % 2)

    def hop(j, h):
        mine = pair_of(j) + k
        pieces = pl.ds(h * piece, piece)
        came = [p == 1, None, z >= 1, z >= 1, (z >= 2) & (k == 1), (z >= 2) & (p == 0)][j]

        @pl.when(came)
        def _():
            pltpu.make_async_copy(hist.at[pieces], wnd.at[mine, pieces], x_recv.at[mine, h]).wait()
            if j == 2:

                @pl.when((z + 1 < depth) & (k == 1))
                def _():
                    x_copy(mine, mine - ROW, h, 3, up).start()

                x_copy(mine, mine, h, 4, partner).start()
            if j == 3:

                @pl.when((z + 1 < depth) & (r == 0))
                def _():
                    x_copy(mine, mine - ROW, h, 11, up).start()

            if j == 4:

                @pl.when(p == 1)
                def _():
                    x_copy(mine, mine, h, 5, partner).start()

            @pl.when(needed(mine, r + 1 - 2 * k))
            def _():
                x_copy(mine, mine, h, (6, None, 7, 8, 9, 10)[j], sibling).start()

    def all_hops(j, first):
        for h in range(first, CHUNKS):
            hop(j, h)

    def sums_across():
        red1().wait_recv()
        part[pl.ds(2 * k, 2)] += buf1[...]
        out2[...] = part[k * 2 + 1 - p].astype(bf16)
        red2().start()

    def sums_up():
        red2().wait_recv()
        part[me_block] += buf2[...].astype(f32)
        out3[...] = part[me_block].astype(bf16)

        def send(d, c):
            red3(d).start()
            return c

        lax.fori_loop(1, depth, send, 0)

    def event(e):
        if e == 0:
            hop(2, 0)
            sums_across()
            all_hops(2, 1)
            all_hops(0, 0)
        if e == 2:
            hop(3, 0)
        if e == 4:
            all_hops(3, 1)
            sums_up()
        if e == 6:
            all_hops(4, 0)
        if e == 8:
            all_hops(5, 0)

    def one(e, carry):
        for at in (0, 2, 4, 6, 8):

            @pl.when(e == at)
            def _():
                event(at)

        m = e % 2
        slot = pair_of(e // 2) + (k + m) % 2

        @pl.when(needed(slot, r))
        def _():
            @pl.when(m == 1)
            def _():
                for h in range(CHUNKS):
                    pieces = pl.ds(h * piece, piece)
                    pltpu.make_async_copy(
                        hist.at[pieces], wnd.at[slot, pieces], x_recv.at[slot, h]
                    ).wait()

            norm = layer_norm(wnd[slot].astype(f32)).astype(bf16)
            kv_s[0] = project(norm, 3)
            kv_s[1] = project(norm, 1)
            attend(kv_s, (z - 2) * ROW + slot)

        return carry

    lax.fori_loop(0, 12, one, 0)

    w_copies[4].wait()
    y = (layer_norm(acc[...]) * u_s[...].astype(f32)).astype(bf16)
    out_ref[...] = (hist[...].astype(f32) + dot(y, w_out[...])).astype(bf16)

    u_c = project(layer_norm(cand[...].astype(f32)).astype(bf16), 0)

    def take(d, c):
        red3(d).wait_recv()
        return c + buf3[d].astype(f32)

    mine_sum = part[me_block, mine_at]
    cattn = lax.fori_loop(1, depth, take, mine_sum)
    y_c = (layer_norm(cattn) * u_c.astype(f32)).astype(bf16)
    cout_ref[...] = (cand[...].astype(f32) + dot(y_c, w_out[...])).astype(bf16)

    for c in to_partner + to_sibling + [red1(), red2()]:
        c.wait_send()

    def left(d, c):
        cz_copy(d, 0).wait_send()
        cz_copy(d, 1).wait_send()
        red3(d).wait_send()
        return c

    lax.fori_loop(1, depth, left, 0)
    for h in range(CHUNKS):

        @pl.when(z + 1 < depth)
        def _():
            x_copy(None, ROW + r, h, 0, up).wait_send()

        @pl.when(p == 0)
        def _():
            x_copy(None, own_slot, h, 1, partner).wait_send()

        @pl.when(k == 0)
        def _():
            x_copy(None, own_slot, h, 2, sibling).wait_send()

        @pl.when((z >= 1) & (z + 1 < depth) & (k == 1))
        def _():
            x_copy(ROW + r, r, h, 3, up).wait_send()

        @pl.when(z >= 1)
        def _():
            x_copy(ROW + r, ROW + r, h, 4, partner).wait_send()

        @pl.when((z >= 2) & (r == 3))
        def _():
            x_copy(r, r, h, 5, partner).wait_send()

        other = r + 1 - 2 * k
        across = 2 * (1 - p) + k

        @pl.when((z >= 1) & (z + 1 < depth) & (r == 0))
        def _():
            x_copy(ROW + across, across, h, 11, up).wait_send()

        for kind, came, slot in (
            (6, p == 1, 2 * ROW + k),
            (7, z >= 1, ROW + r),
            (8, z >= 1, ROW + across),
            (9, (z >= 2) & (k == 1), r),
            (10, (z >= 2) & (p == 0), across),
        ):

            @pl.when(came & needed(slot, other))
            def _():
                x_copy(slot, slot, h, kind, sibling).wait_send()


def per_device(n, history, candidates, lengths, cand_user, w_in, w_out):
    rows, width = history.shape
    cr = candidates.shape[0]
    depth = n // ROW
    users = cand_user[None, :]
    vmem = pl.BlockSpec(memory_space=pltpu.VMEM)
    dma = pltpu.SemaphoreType.DMA
    block = depth * cr
    many = ROW * block if ROW * block <= 512 else block
    return pl.pallas_call(
        functools.partial(kernel, n),
        out_shape=(
            jax.ShapeDtypeStruct((rows, width), bf16),
            jax.ShapeDtypeStruct((cr, width), bf16),
        ),
        in_specs=[
            pl.BlockSpec(memory_space=pltpu.SMEM),
            vmem,
            vmem,
            vmem,
            pl.BlockSpec(memory_space=pl.ANY),
            pl.BlockSpec(memory_space=pl.ANY),
        ],
        out_specs=(vmem, vmem),
        scratch_shapes=[
            pltpu.VMEM((4, width, width), bf16),
            pltpu.VMEM((width, width), bf16),
            pltpu.VMEM((3 * ROW, rows, width), bf16),
            pltpu.VMEM((rows, width), bf16),
            pltpu.VMEM((rows, width), bf16),
            pltpu.VMEM((2, rows, width), bf16),
            pltpu.VMEM((2, rows, width), bf16),
            pltpu.VMEM((rows, width), f32),
            pltpu.VMEM((ROW, block, width), bf16),
            pltpu.VMEM((ROW, block, 128), jnp.int32),
            pltpu.VMEM((many, width), bf16),
            pltpu.VMEM((ROW, block, width), f32),
            pltpu.VMEM((2, block, width), f32),
            pltpu.VMEM((block, width), bf16),
            pltpu.VMEM((depth, cr, width), bf16),
            pltpu.VMEM((block, width), bf16),
            pltpu.VMEM((block, width), bf16),
            pltpu.VMEM((cr, 128), jnp.int32),
            dma((5,)),
            dma((12, CHUNKS)),
            dma((3 * ROW, CHUNKS)),
            dma((depth,)),
            dma((depth,)),
            dma((depth,)),
            dma((depth,)),
            dma((6,)),
            dma((6,)),
            dma((depth,)),
            dma((depth,)),
        ],
        compiler_params=pltpu.CompilerParams(
            collective_id=0, has_side_effects=True, vmem_limit_bytes=60 * 1024 * 1024
        ),
    )(lengths, history, candidates, users, w_in, w_out)


def solution(mesh):
    n = mesh.shape["seq"]
    placed = (
        P(("grp", "seq"), None),
        P(("grp", "seq"), None),
        P("grp"),
        P(("grp", "seq")),
        P(),
        P(),
    )
    return jax.shard_map(
        functools.partial(per_device, n),
        mesh=mesh,
        in_specs=placed,
        out_specs=(P(("grp", "seq"), None), P(("grp", "seq"), None)),
        check_vma=False,
    )
```

```python
import functools

import jax
import jax.numpy as jnp
from jax import lax
from jax.experimental import pallas as pl
from jax.experimental.pallas import tpu as pltpu
from jax.sharding import PartitionSpec as P

HEADS = 8
WIN = 8
CHUNKS = 4
ROW = 4

eps = 1e-06
bf16 = jnp.bfloat16
f32 = jnp.float32


def layer_norm(rows):
    centred = rows - jnp.mean(rows, axis=-1, keepdims=True)
    return centred * lax.rsqrt(jnp.mean(centred * centred, axis=-1, keepdims=True) + eps)


def silu_of_twice(half):
    return half + half * jnp.tanh(half)


def dot(a, b):
    return jnp.dot(a, b, preferred_element_type=f32)


def dot_t(a, b):
    return lax.dot_general(a, b, (((1,), (1,)), ((), ())), preferred_element_type=f32)


def kernel(
    n,
    lengths,
    hist,
    cand,
    users_row,
    w_in_hbm,
    w_out_hbm,
    out_ref,
    cout_ref,
    w_in,
    w_out,
    wnd,
    q_s,
    u_s,
    kv_s,
    own_kv,
    acc,
    cbuf,
    ubuf,
    qc_s,
    part,
    buf1,
    buf2,
    buf3,
    out2,
    out3,
    users,
    uc_s,
    w_sem,
    x_send,
    x_recv,
    cz_send,
    cz_recv,
    uz_send,
    uz_recv,
    cx_send,
    cx_recv,
    rz_send,
    rz_recv,
):
    rows, width = hist.shape
    cr = cand.shape[0]
    head_dim = width // HEADS
    half_scale = 0.5 * head_dim ** (-0.5)
    depth = n // ROW
    s = lax.axis_index("seq")
    z = s // ROW
    r = s % ROW
    p = r // 2
    k = r % 2
    piece = rows // CHUNKS
    sibling = s + 1 - 2 * k
    partner = s + 2 - 4 * p

    w_copies = [
        pltpu.make_async_copy(
            w_in_hbm.at[0, :, pl.ds(c * width, width)], w_in.at[c], w_sem.at[c]
        )
        for c in range(4)
    ]
    w_copies.append(pltpu.make_async_copy(w_out_hbm.at[0], w_out, w_sem.at[4]))
    for c in (2, 3, 1, 0, 4):
        w_copies[c].start()

    eye = lax.broadcasted_iota(jnp.int32, (cr, cr), 0) == lax.broadcasted_iota(jnp.int32, (cr, cr), 1)
    column = jnp.sum(jnp.where(eye, users_row[...], 0), axis=1, keepdims=True)
    users[...] = jnp.broadcast_to(column, users.shape)

    barrier = pltpu.get_barrier_semaphore()
    pl.semaphore_signal(barrier, inc=1, device_id={"seq": sibling}, device_id_type=pl.DeviceIdType.MESH)
    pl.semaphore_signal(barrier, inc=1, device_id={"seq": partner}, device_id_type=pl.DeviceIdType.MESH)

    def greet(d, carry):
        pl.semaphore_signal(
            barrier,
            inc=1,
            device_id={"seq": (s + ROW * d) % n},
            device_id_type=pl.DeviceIdType.MESH,
        )
        return carry

    lax.fori_loop(1, depth, greet, 0)
    own_slot = 2 * ROW + r
    normed = layer_norm(hist[...].astype(f32)).astype(bf16)
    wnd[own_slot] = normed
    pl.semaphore_wait(barrier, depth + 1)

    def remote(src, dst, send, recv, to):
        return pltpu.make_async_remote_copy(
            src_ref=src,
            dst_ref=dst,
            send_sem=send,
            recv_sem=recv,
            device_id={"seq": to},
            device_id_type=pl.DeviceIdType.MESH,
        )

    def x_copy(src_slot, dst_slot, h, kind, to):
        part_rows = pl.ds(h * piece, piece)
        return remote(wnd.at[src_slot, part_rows], wnd.at[dst_slot, part_rows], x_send.at[kind, h], x_recv.at[dst_slot, h], to)

    up = (s + ROW) % n

    me_block = k * 2 + p

    def cz_copy(d, which):
        to = (s + ROW * d) % n
        at = pl.ds(pl.multiple_of(z * cr, cr), cr)
        if which == 0:
            return remote(cand, cbuf.at[me_block, at], cz_send.at[d], cz_recv.at[d], to)
        return remote(users, ubuf.at[me_block, at], uz_send.at[d], uz_recv.at[d], to)

    def cz_start(d, carry):
        cz_copy(d, 0).start()
        cz_copy(d, 1).start()
        return carry

    lax.fori_loop(1, depth, cz_start, 0)

    for h in range(CHUNKS):

        @pl.when(z + 1 < depth)
        def _():
            x_copy(own_slot, ROW + r, h, 0, up).start()

        if h == 0:

            @pl.when(p == 0)
            def _():
                x_copy(own_slot, own_slot, h, 1, partner).start()

        @pl.when(k == 0)
        def _():
            x_copy(own_slot, own_slot, h, 2, sibling).start()

    ends = []
    total = jnp.int32(0)
    for j in range(lengths.shape[0]):
        total = total + lengths[j]
        ends.append(total)

    def seg(pos):
        out = jnp.zeros(pos.shape, jnp.int32)
        for e in ends:
            out = out + (pos >= e).astype(jnp.int32)
        return out

    q_pos = s * rows + lax.broadcasted_iota(jnp.int32, (rows, 1), 0)
    q_seg = seg(q_pos)

    def project(normed, block):
        return silu_of_twice(dot(normed, w_in[block]) * 0.5).astype(bf16)

    def attend(kv, shard):
        k_pos = shard * rows + lax.broadcasted_iota(jnp.int32, (1, rows), 1)
        ok = (k_pos <= q_pos) & (q_pos - k_pos < (WIN - 1) * rows) & (seg(k_pos) == q_seg)
        for h in range(HEADS):
            cols = slice(h * head_dim, (h + 1) * head_dim)
            half = dot_t(q_s[:, cols], kv[0, :, cols]) * half_scale
            weight = jnp.where(ok, silu_of_twice(half), 0.0).astype(bf16)
            acc[:, cols] += dot(weight, kv[1, :, cols])

    def needed(slot, of):
        return (slot > of) & (slot < 2 * ROW + of) & (z - 2 + slot // ROW >= 0)

    def pair_of(j):
        base = 2 * ROW - ROW * (j // 2)
        swap = min(j // 2, 1) * p if isinstance(j, int) else jnp.minimum(j // 2, 1) * p
        return base + 2 * ((j + swap) % 2)

    def hop(j, h):
        mine = pair_of(j) + k
        pieces = pl.ds(h * piece, piece)
        came = [p == 1, None, z >= 1, z >= 1, (z >= 2) & (k == 1), (z >= 2) & (p == 0)][j]

        @pl.when(came)
        def _():
            pltpu.make_async_copy(hist.at[pieces], wnd.at[mine, pieces], x_recv.at[mine, h]).wait()
            if j == 2:

                @pl.when((z + 1 < depth) & (k == 1))
                def _():
                    x_copy(mine, mine - ROW, h, 3, up).start()

                x_copy(mine, mine, h, 4, partner).start()
            if j == 3:

                @pl.when((z + 1 < depth) & (r == 0))
                def _():
                    x_copy(mine, mine - ROW, h, 11, up).start()

            if j == 4:

                @pl.when(p == 1)
                def _():
                    x_copy(mine, mine, h, 5, partner).start()

            @pl.when(needed(mine, r + 1 - 2 * k))
            def _():
                x_copy(mine, mine, h, (6, None, 7, 8, 9, 10)[j], sibling).start()

    def all_hops(j, first):
        for h in range(first, CHUNKS):
            hop(j, h)

    acc[...] = jnp.zeros_like(acc)
    mine_at = pl.ds(pl.multiple_of(z * cr, cr), cr)
    cbuf[me_block, mine_at] = cand[...]
    ubuf[me_block, mine_at] = users[...]
    w_copies[2].wait()
    q_s[...] = project(normed, 2)
    w_copies[3].wait()
    own_kv[0] = project(normed, 3)
    w_copies[1].wait()
    own_kv[1] = project(normed, 1)

    def cz_wait(d, carry):
        cz_copy(d, 0).wait_recv()
        cz_copy(d, 1).wait_recv()
        return carry

    lax.fori_loop(1, depth, cz_wait, 0)
    to_partner = [
        remote(cbuf.at[me_block], cbuf.at[me_block], cx_send.at[0], cx_recv.at[0], partner),
        remote(ubuf.at[me_block], ubuf.at[me_block], cx_send.at[1], cx_recv.at[1], partner),
    ]
    for c in to_partner:
        c.start()
    for h in range(1, CHUNKS):

        @pl.when(p == 0)
        def _():
            x_copy(own_slot, own_slot, h, 1, partner).start()

    hop(2, 0)
    w_copies[0].wait()
    u_s[...] = project(normed, 0)
    attend(own_kv, s)
    hop(2, 1)
    for c in to_partner:
        c.wait_recv()
    to_sibling = [
        remote(cbuf.at[pl.ds(2 * k, 2)], cbuf.at[pl.ds(2 * k, 2)], cx_send.at[2], cx_recv.at[2], sibling),
        remote(ubuf.at[pl.ds(2 * k, 2)], ubuf.at[pl.ds(2 * k, 2)], cx_send.at[3], cx_recv.at[3], sibling),
    ]
    for c in to_sibling:
        c.start()
    u_c = project(layer_norm(cand[...].astype(f32)).astype(bf16), 0)
    uc_s[...] = u_c
    hop(2, 2)
    for c in to_sibling:
        c.wait_recv()

    def red1():
        return remote(part.at[pl.ds(2 - 2 * k, 2)], buf1, cx_send.at[4], cx_recv.at[4], sibling)

    def red2():
        return remote(out2, buf2, cx_send.at[5], cx_recv.at[5], partner)

    def red3(d):
        to_row = (z + d) % depth
        src = out3.at[pl.ds(pl.multiple_of(to_row * cr, cr), cr)]
        return remote(src, buf3.at[d], rz_send.at[d], rz_recv.at[d], (s + ROW * d) % n)

    block_rows = depth * cr
    k_row = s * rows + lax.broadcasted_iota(jnp.int32, (1, rows), 1)
    k_seg = seg(k_row)

    def cand_scores(first, count):
        size = count * block_rows
        c_norm = layer_norm(cbuf[pl.ds(first, count)].reshape(size, width).astype(f32)).astype(bf16)
        qc_s[...] = project(c_norm, 2)
        owner = ubuf[pl.ds(first, count)].reshape(size, ubuf.shape[-1])[:, :1]
        ok = owner == k_seg
        for h in range(HEADS):
            cols = slice(h * head_dim, (h + 1) * head_dim)
            half = dot_t(qc_s[:, cols], own_kv[0, :, cols]) * half_scale
            weight = jnp.where(ok, silu_of_twice(half), 0.0).astype(bf16)
            part[pl.ds(first, count), :, cols] = dot(weight, own_kv[1, :, cols]).reshape(
                count, block_rows, head_dim
            )

    count = qc_s.shape[0] // block_rows
    if count == ROW:
        cand_scores(0, ROW)
    else:

        def cand_block(b, carry):
            cand_scores(b * count, count)
            return carry

        lax.fori_loop(0, ROW // count, cand_block, 0)
    red1().start()

    def sums_across():
        red1().wait_recv()
        part[pl.ds(2 * k, 2)] += buf1[...]
        out2[...] = part[k * 2 + 1 - p].astype(bf16)
        red2().start()

    def sums_up():
        red2().wait_recv()
        part[me_block] += buf2[...].astype(f32)
        out3[...] = part[me_block].astype(bf16)

        def send(d, c):
            red3(d).start()
            return c

        lax.fori_loop(1, depth, send, 0)

    def event(e):
        if e == 0:
            hop(2, 3)
            sums_across()
        if e == 2:
            all_hops(0, 0)
        if e == 5:
            sums_up()
        for j, h in {2: ((3, 0),), 3: ((3, 1),), 4: ((3, 2), (4, 0)), 5: ((3, 3), (4, 1)), 6: ((4, 2),), 7: ((4, 3),), 8: ((5, 0), (5, 1)), 9: ((5, 2),), 10: ((5, 3),)}.get(e, ()):
            hop(j, h)

    def one(e, carry):
        for at in (0, 2, 3, 4, 5, 6, 7, 8, 9, 10):

            @pl.when(e == at)
            def _():
                event(at)

        step = e // 2
        late = jnp.minimum(step // 3, 1)
        j = (1 - late) * ((step + 2) % 3) + late * step
        m = e % 2
        slot = pair_of(j) + (k + m) % 2

        @pl.when(needed(slot, r))
        def _():
            @pl.when(m == 1)
            def _():
                for h in range(CHUNKS):
                    pieces = pl.ds(h * piece, piece)
                    pltpu.make_async_copy(
                        hist.at[pieces], wnd.at[slot, pieces], x_recv.at[slot, h]
                    ).wait()

            norm = wnd[slot]
            kv_s[0] = project(norm, 3)
            kv_s[1] = project(norm, 1)
            attend(kv_s, (z - 2) * ROW + slot)

        return carry

    lax.fori_loop(0, 12, one, 0)

    w_copies[4].wait()

    def take(d, c):
        red3(d).wait_recv()
        return c + buf3[d].astype(f32)

    cattn = lax.fori_loop(1, depth, take, part[me_block, mine_at])
    y_c = (layer_norm(cattn) * uc_s[...].astype(f32)).astype(bf16)
    y = (layer_norm(acc[...]) * u_s[...].astype(f32)).astype(bf16)
    both = dot(jnp.concatenate([y, y_c], axis=0), w_out[...])
    out_ref[...] = (hist[...].astype(f32) + both[:rows]).astype(bf16)
    cout_ref[...] = (cand[...].astype(f32) + both[rows:]).astype(bf16)

    for c in to_partner + to_sibling + [red1(), red2()]:
        c.wait_send()

    def left(d, c):
        cz_copy(d, 0).wait_send()
        cz_copy(d, 1).wait_send()
        red3(d).wait_send()
        return c

    lax.fori_loop(1, depth, left, 0)
    for h in range(CHUNKS):

        @pl.when(z + 1 < depth)
        def _():
            x_copy(own_slot, ROW + r, h, 0, up).wait_send()

        @pl.when(p == 0)
        def _():
            x_copy(own_slot, own_slot, h, 1, partner).wait_send()

        @pl.when(k == 0)
        def _():
            x_copy(own_slot, own_slot, h, 2, sibling).wait_send()

        @pl.when((z >= 1) & (z + 1 < depth) & (k == 1))
        def _():
            x_copy(ROW + r, r, h, 3, up).wait_send()

        @pl.when(z >= 1)
        def _():
            x_copy(ROW + r, ROW + r, h, 4, partner).wait_send()

        @pl.when((z >= 2) & (r == 3))
        def _():
            x_copy(r, r, h, 5, partner).wait_send()

        other = r + 1 - 2 * k
        across = 2 * (1 - p) + k

        @pl.when((z >= 1) & (z + 1 < depth) & (r == 0))
        def _():
            x_copy(ROW + across, across, h, 11, up).wait_send()

        for kind, came, slot in (
            (6, p == 1, 2 * ROW + k),
            (7, z >= 1, ROW + r),
            (8, z >= 1, ROW + across),
            (9, (z >= 2) & (k == 1), r),
            (10, (z >= 2) & (p == 0), across),
        ):

            @pl.when(came & needed(slot, other))
            def _():
                x_copy(slot, slot, h, kind, sibling).wait_send()


def per_device(n, history, candidates, lengths, cand_user, w_in, w_out):
    rows, width = history.shape
    cr = candidates.shape[0]
    depth = n // ROW
    users = cand_user[None, :]
    vmem = pl.BlockSpec(memory_space=pltpu.VMEM)
    dma = pltpu.SemaphoreType.DMA
    block = depth * cr
    many = ROW * block if ROW * block <= 512 else block
    return pl.pallas_call(
        functools.partial(kernel, n),
        out_shape=(
            jax.ShapeDtypeStruct((rows, width), bf16),
            jax.ShapeDtypeStruct((cr, width), bf16),
        ),
        in_specs=[
            pl.BlockSpec(memory_space=pltpu.SMEM),
            vmem,
            vmem,
            vmem,
            pl.BlockSpec(memory_space=pl.ANY),
            pl.BlockSpec(memory_space=pl.ANY),
        ],
        out_specs=(vmem, vmem),
        scratch_shapes=[
            pltpu.VMEM((4, width, width), bf16),
            pltpu.VMEM((width, width), bf16),
            pltpu.VMEM((3 * ROW, rows, width), bf16),
            pltpu.VMEM((rows, width), bf16),
            pltpu.VMEM((rows, width), bf16),
            pltpu.VMEM((2, rows, width), bf16),
            pltpu.VMEM((2, rows, width), bf16),
            pltpu.VMEM((rows, width), f32),
            pltpu.VMEM((ROW, block, width), bf16),
            pltpu.VMEM((ROW, block, 128), jnp.int32),
            pltpu.VMEM((many, width), bf16),
            pltpu.VMEM((ROW, block, width), f32),
            pltpu.VMEM((2, block, width), f32),
            pltpu.VMEM((block, width), bf16),
            pltpu.VMEM((depth, cr, width), bf16),
            pltpu.VMEM((block, width), bf16),
            pltpu.VMEM((block, width), bf16),
            pltpu.VMEM((cr, 128), jnp.int32),
            pltpu.VMEM((cr, width), bf16),
            dma((5,)),
            dma((12, CHUNKS)),
            dma((3 * ROW, CHUNKS)),
            dma((depth,)),
            dma((depth,)),
            dma((depth,)),
            dma((depth,)),
            dma((6,)),
            dma((6,)),
            dma((depth,)),
            dma((depth,)),
        ],
        compiler_params=pltpu.CompilerParams(
            collective_id=0, has_side_effects=True, vmem_limit_bytes=60 * 1024 * 1024
        ),
    )(lengths, history, candidates, users, w_in, w_out)


def solution(mesh):
    n = mesh.shape["seq"]
    placed = (
        P(("grp", "seq"), None),
        P(("grp", "seq"), None),
        P("grp"),
        P(("grp", "seq")),
        P(),
        P(),
    )
    return jax.shard_map(
        functools.partial(per_device, n),
        mesh=mesh,
        in_specs=placed,
        out_specs=(P(("grp", "seq"), None), P(("grp", "seq"), None)),
        check_vma=False,
    )
```

```python
import functools

import jax
import jax.numpy as jnp
from jax import lax
from jax.experimental import pallas as pl
from jax.experimental.pallas import tpu as pltpu
from jax.sharding import PartitionSpec as P

HEADS = 8
WIN = 8
CHUNKS = 4
ROW = 4

eps = 1e-06
bf16 = jnp.bfloat16
f32 = jnp.float32


def layer_norm(rows):
    centred = rows - jnp.mean(rows, axis=-1, keepdims=True)
    return centred * lax.rsqrt(jnp.mean(centred * centred, axis=-1, keepdims=True) + eps)


def silu_of_twice(half):
    return half + half * jnp.tanh(half)


def dot(a, b):
    return jnp.dot(a, b, preferred_element_type=f32)


def dot_t(a, b):
    return lax.dot_general(a, b, (((1,), (1,)), ((), ())), preferred_element_type=f32)


def kernel(
    n,
    lengths,
    hist,
    cand,
    users_row,
    w_in_hbm,
    w_out_hbm,
    out_ref,
    cout_ref,
    w_in,
    w_out,
    wnd,
    q_s,
    u_s,
    kv_s,
    own_kv,
    acc,
    cbuf,
    ubuf,
    qc_s,
    part,
    buf1,
    buf2,
    buf3,
    out2,
    out3,
    users,
    uc_s,
    w_sem,
    x_send,
    x_recv,
    cz_send,
    cz_recv,
    uz_send,
    uz_recv,
    cx_send,
    cx_recv,
    rz_send,
    rz_recv,
):
    rows, width = hist.shape
    cr = cand.shape[0]
    head_dim = width // HEADS
    half_scale = 0.5 * head_dim ** (-0.5)
    depth = n // ROW
    s = lax.axis_index("seq")
    z = s // ROW
    r = s % ROW
    p = r // 2
    k = r % 2
    piece = rows // CHUNKS
    sibling = s + 1 - 2 * k
    partner = s + 2 - 4 * p

    w_copies = [
        pltpu.make_async_copy(
            w_in_hbm.at[0, :, pl.ds(c * width, width)], w_in.at[c], w_sem.at[c]
        )
        for c in range(4)
    ]
    w_copies.append(pltpu.make_async_copy(w_out_hbm.at[0], w_out, w_sem.at[4]))
    for c in (2, 3, 1, 0, 4):
        w_copies[c].start()

    eye = lax.broadcasted_iota(jnp.int32, (cr, cr), 0) == lax.broadcasted_iota(jnp.int32, (cr, cr), 1)
    column = jnp.sum(jnp.where(eye, users_row[...], 0), axis=1, keepdims=True)
    users[...] = jnp.broadcast_to(column, users.shape)

    barrier = pltpu.get_barrier_semaphore()
    pl.semaphore_signal(barrier, inc=1, device_id={"seq": sibling}, device_id_type=pl.DeviceIdType.MESH)
    pl.semaphore_signal(barrier, inc=1, device_id={"seq": partner}, device_id_type=pl.DeviceIdType.MESH)

    def greet(d, carry):
        pl.semaphore_signal(
            barrier,
            inc=1,
            device_id={"seq": (s + ROW * d) % n},
            device_id_type=pl.DeviceIdType.MESH,
        )
        return carry

    lax.fori_loop(1, depth, greet, 0)
    own_slot = 2 * ROW + r
    normed = layer_norm(hist[...].astype(f32)).astype(bf16)
    wnd[own_slot] = normed
    pl.semaphore_wait(barrier, depth + 1)

    def remote(src, dst, send, recv, to):
        return pltpu.make_async_remote_copy(
            src_ref=src,
            dst_ref=dst,
            send_sem=send,
            recv_sem=recv,
            device_id={"seq": to},
            device_id_type=pl.DeviceIdType.MESH,
        )

    def x_copy(src_slot, dst_slot, h, kind, to):
        part_rows = pl.ds(h * piece, piece)
        return remote(wnd.at[src_slot, part_rows], wnd.at[dst_slot, part_rows], x_send.at[kind, h], x_recv.at[dst_slot, h], to)

    up = (s + ROW) % n

    me_block = k * 2 + p

    def cz_copy(d, which):
        to = (s + ROW * d) % n
        at = pl.ds(pl.multiple_of(z * cr, cr), cr)
        if which == 0:
            return remote(cand, cbuf.at[me_block, at], cz_send.at[d], cz_recv.at[d], to)
        return remote(users, ubuf.at[me_block, at], uz_send.at[d], uz_recv.at[d], to)

    def cz_start(d, carry):
        cz_copy(d, 0).start()
        cz_copy(d, 1).start()
        return carry

    lax.fori_loop(1, depth, cz_start, 0)

    for h in range(CHUNKS):

        @pl.when(z + 1 < depth)
        def _():
            x_copy(own_slot, ROW + r, h, 0, up).start()

        if h == 0:

            @pl.when(p == 0)
            def _():
                x_copy(own_slot, own_slot, h, 1, partner).start()

        @pl.when(k == 0)
        def _():
            x_copy(own_slot, own_slot, h, 2, sibling).start()

    ends = []
    total = jnp.int32(0)
    for j in range(lengths.shape[0]):
        total = total + lengths[j]
        ends.append(total)

    def seg(pos):
        out = jnp.zeros(pos.shape, jnp.int32)
        for e in ends:
            out = out + (pos >= e).astype(jnp.int32)
        return out

    q_pos = s * rows + lax.broadcasted_iota(jnp.int32, (rows, 1), 0)
    q_seg = seg(q_pos)

    def project(normed, block):
        return silu_of_twice(dot(normed, w_in[block]) * 0.5).astype(bf16)

    def attend(kv, shard):
        k_pos = shard * rows + lax.broadcasted_iota(jnp.int32, (1, rows), 1)
        ok = (k_pos <= q_pos) & (q_pos - k_pos < (WIN - 1) * rows) & (seg(k_pos) == q_seg)
        for h in range(HEADS):
            cols = slice(h * head_dim, (h + 1) * head_dim)
            half = dot_t(q_s[:, cols], kv[0, :, cols]) * half_scale
            weight = jnp.where(ok, silu_of_twice(half), 0.0).astype(bf16)
            acc[:, cols] += dot(weight, kv[1, :, cols])

    def needed(slot, of):
        return (slot > of) & (slot < 2 * ROW + of) & (z - 2 + slot // ROW >= 0)

    def pair_of(j):
        base = 2 * ROW - ROW * (j // 2)
        swap = min(j // 2, 1) * p if isinstance(j, int) else jnp.minimum(j // 2, 1) * p
        return base + 2 * ((j + swap) % 2)

    def hop(j, h):
        mine = pair_of(j) + k
        pieces = pl.ds(h * piece, piece)
        came = [p == 1, None, z >= 1, z >= 1, (z >= 2) & (k == 1), (z >= 2) & (p == 0)][j]

        @pl.when(came)
        def _():
            pltpu.make_async_copy(hist.at[pieces], wnd.at[mine, pieces], x_recv.at[mine, h]).wait()
            if j == 2:

                @pl.when((z + 1 < depth) & (k == 1))
                def _():
                    x_copy(mine, mine - ROW, h, 3, up).start()

                x_copy(mine, mine, h, 4, partner).start()
            if j == 3:

                @pl.when((z + 1 < depth) & (r == 0))
                def _():
                    x_copy(mine, mine - ROW, h, 11, up).start()

            if j == 4:

                @pl.when(p == 1)
                def _():
                    x_copy(mine, mine, h, 5, partner).start()

            @pl.when(needed(mine, r + 1 - 2 * k))
            def _():
                x_copy(mine, mine, h, (6, None, 7, 8, 9, 10)[j], sibling).start()

    def all_hops(j, first):
        for h in range(first, CHUNKS):
            hop(j, h)

    acc[...] = jnp.zeros_like(acc)
    mine_at = pl.ds(pl.multiple_of(z * cr, cr), cr)
    cbuf[me_block, mine_at] = cand[...]
    ubuf[me_block, mine_at] = users[...]
    w_copies[2].wait()
    q_s[...] = project(normed, 2)
    w_copies[3].wait()
    own_kv[0] = project(normed, 3)
    w_copies[1].wait()
    own_kv[1] = project(normed, 1)

    def cz_wait(d, carry):
        cz_copy(d, 0).wait_recv()
        cz_copy(d, 1).wait_recv()
        return carry

    lax.fori_loop(1, depth, cz_wait, 0)
    to_partner = [
        remote(cbuf.at[me_block], cbuf.at[me_block], cx_send.at[0], cx_recv.at[0], partner),
        remote(ubuf.at[me_block], ubuf.at[me_block], cx_send.at[1], cx_recv.at[1], partner),
    ]
    for c in to_partner:
        c.start()
    for h in range(1, CHUNKS):

        @pl.when(p == 0)
        def _():
            x_copy(own_slot, own_slot, h, 1, partner).start()

    hop(2, 0)
    w_copies[0].wait()
    u_s[...] = project(normed, 0)
    attend(own_kv, s)
    hop(2, 1)
    for c in to_partner:
        c.wait_recv()
    to_sibling = [
        remote(cbuf.at[pl.ds(2 * k, 2)], cbuf.at[pl.ds(2 * k, 2)], cx_send.at[2], cx_recv.at[2], sibling),
        remote(ubuf.at[pl.ds(2 * k, 2)], ubuf.at[pl.ds(2 * k, 2)], cx_send.at[3], cx_recv.at[3], sibling),
    ]
    for c in to_sibling:
        c.start()
    u_c = project(layer_norm(cand[...].astype(f32)).astype(bf16), 0)
    uc_s[...] = u_c
    hop(2, 2)
    for c in to_sibling:
        c.wait_recv()

    def red1():
        return remote(part.at[pl.ds(2 - 2 * k, 2)], buf1, cx_send.at[4], cx_recv.at[4], sibling)

    def red2():
        return remote(out2, buf2, cx_send.at[5], cx_recv.at[5], partner)

    def red3(d):
        to_row = (z + d) % depth
        src = out3.at[pl.ds(pl.multiple_of(to_row * cr, cr), cr)]
        return remote(src, buf3.at[d], rz_send.at[d], rz_recv.at[d], (s + ROW * d) % n)

    block_rows = depth * cr
    k_row = s * rows + lax.broadcasted_iota(jnp.int32, (1, rows), 1)
    k_seg = seg(k_row)

    def cand_scores(first, count):
        size = count * block_rows
        c_norm = layer_norm(cbuf[pl.ds(first, count)].reshape(size, width).astype(f32)).astype(bf16)
        qc_s[...] = project(c_norm, 2)
        owner = ubuf[pl.ds(first, count)].reshape(size, ubuf.shape[-1])[:, :1]
        ok = owner == k_seg
        for h in range(HEADS):
            cols = slice(h * head_dim, (h + 1) * head_dim)
            half = dot_t(qc_s[:, cols], own_kv[0, :, cols]) * half_scale
            weight = jnp.where(ok, silu_of_twice(half), 0.0).astype(bf16)
            part[pl.ds(first, count), :, cols] = dot(weight, own_kv[1, :, cols]).reshape(
                count, block_rows, head_dim
            )

    count = qc_s.shape[0] // block_rows
    if count == ROW:
        cand_scores(0, ROW)
    else:

        def cand_block(b, carry):
            cand_scores(b * count, count)
            return carry

        lax.fori_loop(0, ROW // count, cand_block, 0)
    red1().start()

    def sums_across():
        red1().wait_recv()
        part[pl.ds(2 * k, 2)] += buf1[...]
        out2[...] = part[k * 2 + 1 - p].astype(bf16)
        red2().start()

    def sums_up():
        red2().wait_recv()
        part[me_block] += buf2[...].astype(f32)
        out3[...] = part[me_block].astype(bf16)

        def send(d, c):
            red3(d).start()
            return c

        lax.fori_loop(1, depth, send, 0)

    def event(e):
        if e == 0:
            hop(2, 3)
        if e == 1:
            sums_across()
        if e == 2:
            all_hops(0, 0)
        if e == 7:
            sums_up()
        for j, h in {2: ((3, 0),), 3: ((3, 1), (4, 0)), 4: ((3, 2), (4, 1)), 5: ((3, 3), (4, 2)), 6: ((4, 3),), 7: ((5, 0),), 8: ((5, 1),), 9: ((5, 2),), 10: ((5, 3),)}.get(e, ()):
            hop(j, h)

    def one(e, carry):
        for at in (0, 1, 2, 3, 4, 5, 6, 7, 8, 9, 10):

            @pl.when(e == at)
            def _():
                event(at)

        step = e // 2
        late = jnp.minimum(step // 3, 1)
        j = (1 - late) * ((step + 2) % 3) + late * step
        m = e % 2
        slot = pair_of(j) + (k + m) % 2

        @pl.when(needed(slot, r))
        def _():
            @pl.when(m == 1)
            def _():
                for h in range(CHUNKS):
                    pieces = pl.ds(h * piece, piece)
                    pltpu.make_async_copy(
                        hist.at[pieces], wnd.at[slot, pieces], x_recv.at[slot, h]
                    ).wait()

            norm = wnd[slot]
            kv_s[0] = project(norm, 3)
            kv_s[1] = project(norm, 1)
            attend(kv_s, (z - 2) * ROW + slot)

        return carry

    lax.fori_loop(0, 12, one, 0)

    w_copies[4].wait()

    def take(d, c):
        red3(d).wait_recv()
        return c + buf3[d].astype(f32)

    cattn = lax.fori_loop(1, depth, take, part[me_block, mine_at])
    y_c = (layer_norm(cattn) * uc_s[...].astype(f32)).astype(bf16)
    y = (layer_norm(acc[...]) * u_s[...].astype(f32)).astype(bf16)
    both = dot(jnp.concatenate([y, y_c], axis=0), w_out[...])
    out_ref[...] = (hist[...].astype(f32) + both[:rows]).astype(bf16)
    cout_ref[...] = (cand[...].astype(f32) + both[rows:]).astype(bf16)

    for c in to_partner + to_sibling + [red1(), red2()]:
        c.wait_send()

    def left(d, c):
        cz_copy(d, 0).wait_send()
        cz_copy(d, 1).wait_send()
        red3(d).wait_send()
        return c

    lax.fori_loop(1, depth, left, 0)
    for h in range(CHUNKS):

        @pl.when(z + 1 < depth)
        def _():
            x_copy(own_slot, ROW + r, h, 0, up).wait_send()

        @pl.when(p == 0)
        def _():
            x_copy(own_slot, own_slot, h, 1, partner).wait_send()

        @pl.when(k == 0)
        def _():
            x_copy(own_slot, own_slot, h, 2, sibling).wait_send()

        @pl.when((z >= 1) & (z + 1 < depth) & (k == 1))
        def _():
            x_copy(ROW + r, r, h, 3, up).wait_send()

        @pl.when(z >= 1)
        def _():
            x_copy(ROW + r, ROW + r, h, 4, partner).wait_send()

        @pl.when((z >= 2) & (r == 3))
        def _():
            x_copy(r, r, h, 5, partner).wait_send()

        other = r + 1 - 2 * k
        across = 2 * (1 - p) + k

        @pl.when((z >= 1) & (z + 1 < depth) & (r == 0))
        def _():
            x_copy(ROW + across, across, h, 11, up).wait_send()

        for kind, came, slot in (
            (6, p == 1, 2 * ROW + k),
            (7, z >= 1, ROW + r),
            (8, z >= 1, ROW + across),
            (9, (z >= 2) & (k == 1), r),
            (10, (z >= 2) & (p == 0), across),
        ):

            @pl.when(came & needed(slot, other))
            def _():
                x_copy(slot, slot, h, kind, sibling).wait_send()


def per_device(n, history, candidates, lengths, cand_user, w_in, w_out):
    rows, width = history.shape
    cr = candidates.shape[0]
    depth = n // ROW
    users = cand_user[None, :]
    vmem = pl.BlockSpec(memory_space=pltpu.VMEM)
    dma = pltpu.SemaphoreType.DMA
    block = depth * cr
    many = ROW * block if ROW * block <= 512 else block
    return pl.pallas_call(
        functools.partial(kernel, n),
        out_shape=(
            jax.ShapeDtypeStruct((rows, width), bf16),
            jax.ShapeDtypeStruct((cr, width), bf16),
        ),
        in_specs=[
            pl.BlockSpec(memory_space=pltpu.SMEM),
            vmem,
            vmem,
            vmem,
            pl.BlockSpec(memory_space=pl.ANY),
            pl.BlockSpec(memory_space=pl.ANY),
        ],
        out_specs=(vmem, vmem),
        scratch_shapes=[
            pltpu.VMEM((4, width, width), bf16),
            pltpu.VMEM((width, width), bf16),
            pltpu.VMEM((3 * ROW, rows, width), bf16),
            pltpu.VMEM((rows, width), bf16),
            pltpu.VMEM((rows, width), bf16),
            pltpu.VMEM((2, rows, width), bf16),
            pltpu.VMEM((2, rows, width), bf16),
            pltpu.VMEM((rows, width), f32),
            pltpu.VMEM((ROW, block, width), bf16),
            pltpu.VMEM((ROW, block, 128), jnp.int32),
            pltpu.VMEM((many, width), bf16),
            pltpu.VMEM((ROW, block, width), f32),
            pltpu.VMEM((2, block, width), f32),
            pltpu.VMEM((block, width), bf16),
            pltpu.VMEM((depth, cr, width), bf16),
            pltpu.VMEM((block, width), bf16),
            pltpu.VMEM((block, width), bf16),
            pltpu.VMEM((cr, 128), jnp.int32),
            pltpu.VMEM((cr, width), bf16),
            dma((5,)),
            dma((12, CHUNKS)),
            dma((3 * ROW, CHUNKS)),
            dma((depth,)),
            dma((depth,)),
            dma((depth,)),
            dma((depth,)),
            dma((6,)),
            dma((6,)),
            dma((depth,)),
            dma((depth,)),
        ],
        compiler_params=pltpu.CompilerParams(
            collective_id=0, has_side_effects=True, vmem_limit_bytes=60 * 1024 * 1024
        ),
    )(lengths, history, candidates, users, w_in, w_out)


def solution(mesh):
    n = mesh.shape["seq"]
    placed = (
        P(("grp", "seq"), None),
        P(("grp", "seq"), None),
        P("grp"),
        P(("grp", "seq")),
        P(),
        P(),
    )
    return jax.shard_map(
        functools.partial(per_device, n),
        mesh=mesh,
        in_specs=placed,
        out_specs=(P(("grp", "seq"), None), P(("grp", "seq"), None)),
        check_vma=False,
    )
```
